32 devices in a mesh: rows: 2 (over y), cols: 4 (over z), slabs: 4 (over x, core).
Axes of the slice: x: 2, y: 2, z: 4, core: 2. Of those that a mesh axis runs over, the one named last changes fastest.
Arguments:
- field_values: float32 [8, 256, 256, 128], P('rows', 'cols', 'slabs'), may hold values from 0.2 to 1.8
- mobility: float32 [8, 256, 256, 128], P('rows', 'cols', 'slabs'), may hold values from 0.03 to 0.15
- source: float32 [8, 256, 256, 128], P('rows', 'cols', 'slabs'), may hold values from -0.2 to 0.2
Outputs:
- column_sum: float32 [8, 256, 256, 128], P('rows', 'cols', 'slabs')
- field_values_end: float32 [8, 256, 256, 128], P('rows', 'cols', 'slabs')
The draws below stay inside these ranges and needn't reach their ends.
All inputs are finite; a program needn't handle non-finite values.
Results may differ from the reference program's by a relative error of at most 0.00002.
Values sent between devices are 32-bit elements; how exact they have to be, the bound alone decides.
A program may use at most 320 MiB of HBM per device.

```python
import jax
import jax.numpy as jnp
from jax import lax

GRID_J = 8
GRID_I = 256
GRID_K = 256
MEMBERS = 128
STEPS = 4


def shard_levels(stream_key, shape, split, low, top_value):
    gain = 1.0
    for position, shards_of in split:
        steps = jax.random.uniform(jax.random.fold_in(jax.random.fold_in(stream_key, 6), position), (shards_of,), jnp.float32, low / len(split), top_value / len(split))
        gain = gain * jnp.repeat(jnp.exp(steps), shape[position] // shards_of).reshape((-1,) + (1,) * (len(shape) - 1 - position))
    return gain


def setup_inputs(seed: int = 0) -> dict:
    streams_of = jax.random.split(jax.random.key(seed), 4)
    return {
        "field_values": jnp.clip(0.2 + 1.5999999 * jax.random.uniform(streams_of[0], (GRID_J, GRID_I, GRID_K, MEMBERS), jnp.float32) ** shard_levels(streams_of[0], (GRID_J, GRID_I, GRID_K, MEMBERS), ((0, 2), (1, 4), (2, 4)), -0.2, 0.2), 0.2, 1.8),
        "mobility": jnp.clip(0.03 + 0.120000007 * jax.random.uniform(streams_of[1], (GRID_J, GRID_I, GRID_K, MEMBERS), jnp.float32) ** shard_levels(streams_of[1], (GRID_J, GRID_I, GRID_K, MEMBERS), ((0, 2), (1, 4), (2, 4)), -0.2, 0.2), 0.03, 0.15),
        "source": jnp.clip(jax.random.uniform(streams_of[2], (GRID_J, GRID_I, GRID_K, MEMBERS), jnp.float32, -0.2, 0.2) * shard_levels(streams_of[2], (GRID_J, GRID_I, GRID_K, MEMBERS), ((0, 2), (1, 4), (2, 4)), -0.4, 0.0), -0.2, 0.2),
    }


def strip_edges(values, dims):
    for dim in dims:
        values = lax.slice_in_dim(values, 1, values.shape[dim] - 1, axis=dim)
    return values


def neighbour(values, dim, start, dims):
    others = [other for other in dims if other != dim]
    values = strip_edges(values, others)
    return lax.slice_in_dim(values, start, start + values.shape[dim] - 2, axis=dim)


def one_step(padded, mobility, source):
    middle = strip_edges(padded, (0, 1, 2))
    lower = [neighbour(padded, dim, 0, (0, 1, 2)) for dim in (0, 1, 2)]
    upper = [neighbour(padded, dim, 2, (0, 1, 2)) for dim in (0, 1, 2)]
    spread = lower[0] + upper[0] + lower[1] + upper[1] + lower[2] + upper[2] - 6.0 * middle
    return middle + mobility * spread + source


def reference(field_values, mobility, source):
    for step in range(STEPS):
        field_values = one_step(jnp.pad(field_values, ((1, 1), (1, 1), (1, 1), (0, 0)), mode="constant"), mobility, source)
    column_sum = jnp.cumsum(field_values, axis=0) / GRID_J
    return column_sum, field_values
```

```python
import functools
import math

import jax
import jax.numpy as jnp
from jax import lax
from jax.experimental import pallas as pl
from jax.experimental.pallas import tpu as pltpu
from jax.sharding import PartitionSpec as P

STEPS = 4
MESH = pl.DeviceIdType.MESH


def kernel(counts, chunk, f_in, m_in, s_in, cs_out, f_out, fb, mb, sb, rhalo, khalo, ksend, row_send, row_recv, i_send, i_recv, k_send, k_recv, load_sem, out_sem):
    n_rows, n_cols, n_slabs = counts
    nj, ni, nk, lanes = f_in.shape
    n_chunks = ni // chunk
    scale = 1.0 / (nj * n_rows)
    r, c, s = (lax.axis_index(name) for name in ("rows", "cols", "slabs"))
    up, down, left, right = c > 0, c < n_cols - 1, s > 0, s < n_slabs - 1
    edge = jnp.where(r == 0, nj - 1, 0)
    is_low = (r == 0).astype(jnp.float32)
    is_high = (r == 1).astype(jnp.float32)
    peer = {"rows": 1 - r}
    beside = (
        (up, {"cols": c - 1}),
        (down, {"cols": c + 1}),
        (left, {"slabs": s - 1}),
        (right, {"slabs": s + 1}),
    )

    loads = [
        pltpu.make_async_copy(f_in, fb.at[0, :, pl.ds(1, ni)], load_sem.at[0]),
        pltpu.make_async_copy(m_in, mb, load_sem.at[1]),
        pltpu.make_async_copy(s_in, sb, load_sem.at[2]),
    ]
    for load in loads:
        load.start()

    barrier = pltpu.get_barrier_semaphore()
    pl.semaphore_signal(barrier, inc=1, device_id=peer, device_id_type=MESH)
    for there, device in beside:

        @pl.when(there)
        def _(device=device):
            pl.semaphore_signal(barrier, inc=1, device_id=device, device_id_type=MESH)

    arrivals = 1 + sum(there.astype(jnp.int32) for there, _ in beside)
    pl.semaphore_wait(barrier, arrivals)

    def rows_of(k):
        return pl.ds(k * chunk, chunk)

    def remote(src, dst, send, recv, device):
        return pltpu.make_async_remote_copy(src_ref=src, dst_ref=dst, send_sem=send, recv_sem=recv, device_id=device, device_id_type=MESH)

    def row_copy(src, t, k):
        return remote(src, rhalo.at[t, rows_of(k)], row_send.at[t, k], row_recv.at[t, k], peer)

    def boundary(t, k):
        return fb.at[lax.rem(t, 2), edge, pl.ds(1 + k * chunk, chunk)]

    def i_first(t, src=None):
        p = lax.rem(t, 2)
        src = fb.at[p, :, 1] if src is None else src
        return remote(src, fb.at[p, :, ni + 1], i_send.at[t, 0], i_recv.at[t, 1], {"cols": c - 1})

    def i_last(t, src=None):
        p = lax.rem(t, 2)
        src = fb.at[p, :, ni] if src is None else src
        return remote(src, fb.at[p, :, 0], i_send.at[t, 1], i_recv.at[t, 0], {"cols": c + 1})

    def k_first(t):
        return remote(ksend.at[t, 0], khalo.at[t, 1], k_send.at[t, 0], k_recv.at[t, 1], {"slabs": s - 1})

    def k_last(t):
        return remote(ksend.at[t, 1], khalo.at[t, 0], k_send.at[t, 1], k_recv.at[t, 0], {"slabs": s + 1})

    def first_send(k, carry):
        row_copy(f_in.at[edge, rows_of(k)], 0, k).start()
        return carry

    lax.fori_loop(0, n_chunks, first_send, 0)

    @pl.when(up)
    def _():
        i_first(0, f_in.at[:, 0]).start()

    @pl.when(down)
    def _():
        i_last(0, f_in.at[:, ni - 1]).start()

    for there, place in ((up, 0), (down, ni + 1)):

        @pl.when(jnp.logical_not(there))
        def _(place=place):
            for p in range(2):
                fb[p, :, place] = jnp.zeros((nj, nk, lanes), jnp.float32)

    for there, side in ((left, 0), (right, 1)):

        @pl.when(jnp.logical_not(there))
        def _(side=side):
            def clear(t, carry):
                khalo[t, side] = jnp.zeros((nj, ni, lanes), jnp.float32)
                return carry

            lax.fori_loop(0, STEPS, clear, 0)

    loads[0].wait()

    def first_edges(i, carry):
        for j in range(nj):
            ksend[0, 0, j, pl.ds(i, 1), :] = fb[0, j, i + 1, 0:1, :]
            ksend[0, 1, j, pl.ds(i, 1), :] = fb[0, j, i + 1, nk - 1 : nk, :]
        return carry

    lax.fori_loop(0, ni, first_edges, 0)

    def send_k(t):
        @pl.when(left)
        def _():
            k_first(t).start()

        @pl.when(right)
        def _():
            k_last(t).start()

    send_k(0)
    loads[1].wait()
    loads[2].wait()

    place = lax.broadcasted_iota(jnp.int32, (nk, lanes), 0)
    at_first, at_last = place == 0, place == nk - 1

    def step_chunk(t, k, final):
        p = lax.rem(t, 2)
        q = 1 - p
        row_copy(boundary(t, k), t, k).wait_recv()

        @pl.when(jnp.logical_and(k == 0, up))
        def _():
            i_last(t).wait_recv()

        @pl.when(jnp.logical_and(k == 0, left))
        def _():
            k_last(t).wait_recv()

        @pl.when(jnp.logical_and(k == 0, right))
        def _():
            k_first(t).wait_recv()

        @pl.when(jnp.logical_and(k == n_chunks - 1, down))
        def _():
            i_first(t).wait_recv()

        @pl.when(t >= 1)
        def _():
            row_copy(boundary(t - 1, k), t - 1, k).wait_send()

        @pl.when(jnp.logical_and(t >= 1, jnp.logical_and(k == 0, up)))
        def _():
            i_first(t - 1).wait_send()

        @pl.when(jnp.logical_and(t >= 1, jnp.logical_and(k == n_chunks - 1, down)))
        def _():
            i_last(t - 1).wait_send()

        def one_row(n, carry):
            i = k * chunk + n
            halo = rhalo[t, i]
            total = None
            for j in range(nj):
                x = fb[p, j, i + 1]
                before = fb[p, j - 1, i + 1] if j > 0 else halo * is_high
                after = fb[p, j + 1, i + 1] if j < nj - 1 else halo * is_low
                k_before = jnp.where(at_first, khalo[t, 0, j, pl.ds(i, 1), :], pltpu.roll(x, 1, 0))
                k_after = jnp.where(at_last, khalo[t, 1, j, pl.ds(i, 1), :], pltpu.roll(x, nk - 1, 0))
                spread = before + after + fb[p, j, i] + fb[p, j, i + 2] + k_before + k_after - 6.0 * x
                new = x + mb[j, i] * spread + sb[j, i]
                fb[q, j, i + 1] = new
                if final:
                    total = new if total is None else total + new
                    sb[j, i] = total * scale
                else:
                    ksend[t + 1, 0, j, pl.ds(i, 1), :] = new[0:1]
                    ksend[t + 1, 1, j, pl.ds(i, 1), :] = new[nk - 1 : nk]
            return carry

        lax.fori_loop(0, chunk, one_row, 0)

    def step(t, carry):
        def lap(k, carry):
            step_chunk(t, k, False)
            row_copy(boundary(t + 1, k), t + 1, k).start()

            @pl.when(jnp.logical_and(k == 0, up))
            def _():
                i_first(t + 1).start()

            @pl.when(jnp.logical_and(k == n_chunks - 1, down))
            def _():
                i_last(t + 1).start()

            return carry

        lax.fori_loop(0, n_chunks, lap, 0)
        send_k(t + 1)
        return carry

    lax.fori_loop(0, STEPS - 1, step, 0)

    last = STEPS - 1
    end = STEPS % 2

    def sums_out(k):
        return pltpu.make_async_copy(sb.at[:, rows_of(k)], cs_out.at[:, rows_of(k)], out_sem.at[0, k])

    def field_out(k):
        return pltpu.make_async_copy(fb.at[end, :, pl.ds(1 + k * chunk, chunk)], f_out.at[:, rows_of(k)], out_sem.at[1, k])

    def total_copy(k):
        return row_copy(sb.at[nj - 1, rows_of(k)], STEPS, k)

    def last_lap(k, carry):
        step_chunk(last, k, True)

        @pl.when(r == 0)
        def _():
            total_copy(k).start()
            sums_out(k).start()

        field_out(k).start()
        return carry

    lax.fori_loop(0, n_chunks, last_lap, 0)

    def drain(k, carry):
        row_copy(boundary(last, k), last, k).wait_send()
        field_out(k).wait()
        return carry

    lax.fori_loop(0, n_chunks, drain, 0)

    @pl.when(up)
    def _():
        i_first(last).wait_send()

    @pl.when(down)
    def _():
        i_last(last).wait_send()

    def drain_k(t, carry):
        @pl.when(left)
        def _():
            k_first(t).wait_send()

        @pl.when(right)
        def _():
            k_last(t).wait_send()

        return carry

    lax.fori_loop(0, STEPS, drain_k, 0)

    @pl.when(r == 0)
    def _():
        def finish(k, carry):
            total_copy(k).wait_send()
            sums_out(k).wait()
            return carry

        lax.fori_loop(0, n_chunks, finish, 0)

    @pl.when(r == 1)
    def _():
        def finish(k, carry):
            total_copy(k).wait_recv()

            def add_row(n, carry):
                i = k * chunk + n
                below = rhalo[STEPS, i]
                for j in range(nj):
                    sb[j, i] = sb[j, i] + below
                return carry

            lax.fori_loop(0, chunk, add_row, 0)
            sums_out(k).start()
            return carry

        lax.fori_loop(0, n_chunks, finish, 0)

        def flush(k, carry):
            sums_out(k).wait()
            return carry

        lax.fori_loop(0, n_chunks, flush, 0)


def fused(counts, field_values, mobility, source):
    nj, ni, nk, lanes = field_values.shape
    chunk = math.gcd(ni, 8)
    n_chunks = ni // chunk
    shape = jax.ShapeDtypeStruct(field_values.shape, jnp.float32)
    dma = pltpu.SemaphoreType.DMA
    return pl.pallas_call(
        functools.partial(kernel, counts, chunk),
        out_shape=(shape, shape),
        in_specs=[pl.BlockSpec(memory_space=pl.ANY)] * 3,
        out_specs=[pl.BlockSpec(memory_space=pl.ANY)] * 2,
        scratch_shapes=[
            pltpu.VMEM((2, nj, ni + 2, nk, lanes), jnp.float32),
            pltpu.VMEM((nj, ni, nk, lanes), jnp.float32),
            pltpu.VMEM((nj, ni, nk, lanes), jnp.float32),
            pltpu.VMEM((STEPS + 1, ni, nk, lanes), jnp.float32),
            pltpu.VMEM((STEPS, 2, nj, ni, lanes), jnp.float32),
            pltpu.VMEM((STEPS, 2, nj, ni, lanes), jnp.float32),
            dma((STEPS + 1, n_chunks)),
            dma((STEPS + 1, n_chunks)),
            dma((STEPS, 2)),
            dma((STEPS, 2)),
            dma((STEPS, 2)),
            dma((STEPS, 2)),
            dma((3,)),
            dma((2, n_chunks)),
        ],
        compiler_params=pltpu.CompilerParams(collective_id=0, has_side_effects=True, vmem_limit_bytes=56 * 1024 * 1024),
    )(field_values, mobility, source)


def padded_2(array, sides, width):
    for axis, dim in sides:
        count, length = (lax.axis_size(axis), array.shape[dim])
        up = [(i, (i + 1) % count) for i in range(count - 1)]
        down = [(j, i) for i, j in up]
        last = lax.slice_in_dim(array, length - width, length, axis=dim)
        first = lax.slice_in_dim(array, 0, width, axis=dim)
        before = lax.ppermute(last, axis, up)
        after = lax.ppermute(first, axis, down)
        array = jnp.concatenate([before, array, after], axis=dim)
    return array


def prefix(array, axis, combine, identity):
    count, index = (lax.axis_size(axis), lax.axis_index(axis))
    everything = lax.all_gather(array, axis)
    start = jnp.broadcast_to(jnp.asarray(identity, array.dtype), array.shape)

    def lap(k, before):
        reached = k < index
        new = combine(before, everything[k])
        return jnp.where(reached, new, before)

    return lax.fori_loop(0, count, lap, start)


def strip_edges(values, dims):
    for dim in dims:
        values = lax.slice_in_dim(values, 1, values.shape[dim] - 1, axis=dim)
    return values


def neighbour(values, dim, start, dims):
    others = [other for other in dims if other != dim]
    values = strip_edges(values, others)
    return lax.slice_in_dim(values, start, start + values.shape[dim] - 2, axis=dim)


def one_step(padded, mobility, source):
    middle = strip_edges(padded, (0, 1, 2))
    lower = [neighbour(padded, dim, 0, (0, 1, 2)) for dim in (0, 1, 2)]
    upper = [neighbour(padded, dim, 2, (0, 1, 2)) for dim in (0, 1, 2)]
    spread = lower[0] + upper[0] + lower[1] + upper[1] + lower[2] + upper[2] - 6.0 * middle
    return middle + mobility * spread + source


def local(field_values, mobility, source):
    for step in range(STEPS):
        padded = padded_2(field_values, (("rows", 0), ("cols", 1), ("slabs", 2)), 1)
        field_values = one_step(padded, mobility, source)
    here = jnp.cumsum(field_values, axis=0)
    total = lax.slice_in_dim(here, here.shape[0] - 1, here.shape[0], axis=0)

    def add_pair(earlier_total, later_total):
        return earlier_total + later_total

    below = prefix(total, "rows", add_pair, jnp.zeros_like(total))
    column_sum = (here + below) / (field_values.shape[0] * lax.axis_size("rows"))
    return (column_sum, field_values)


def solution(mesh):
    in_specs = (
        P("rows", "cols", "slabs", None),
        P("rows", "cols", "slabs", None),
        P("rows", "cols", "slabs", None),
    )
    out_specs = (P("rows", "cols", "slabs", None), P("rows", "cols", "slabs", None))
    if mesh.shape["rows"] == 2:
        body = functools.partial(fused, tuple(mesh.shape[name] for name in ("rows", "cols", "slabs")))
    else:
        body = local
    return jax.shard_map(body, mesh=mesh, in_specs=in_specs, out_specs=out_specs, check_vma=False)
```

```python
import functools
import math

import jax
import jax.numpy as jnp
from jax import lax
from jax.experimental import pallas as pl
from jax.experimental.pallas import tpu as pltpu
from jax.sharding import PartitionSpec as P

STEPS = 4
MESH = pl.DeviceIdType.MESH


def kernel(counts, chunk, f_in, m_in, s_in, sb, mb, fb, rhalo, khalo, ksend, row_send, row_recv, i_send, i_recv, k_send, k_recv, load_sem):
    n_rows, n_cols, n_slabs = counts
    nj, ni, nk, lanes = f_in.shape
    n_chunks = ni // chunk
    scale = 1.0 / (nj * n_rows)
    r, c, s = (lax.axis_index(name) for name in ("rows", "cols", "slabs"))
    up, down, left, right = c > 0, c < n_cols - 1, s > 0, s < n_slabs - 1
    edge = jnp.where(r == 0, nj - 1, 0)
    is_low = (r == 0).astype(jnp.float32)
    is_high = (r == 1).astype(jnp.float32)
    peer = {"rows": 1 - r}
    beside = (
        (up, {"cols": c - 1}),
        (down, {"cols": c + 1}),
        (left, {"slabs": s - 1}),
        (right, {"slabs": s + 1}),
    )

    loads = [
        pltpu.make_async_copy(f_in, fb.at[0, :, pl.ds(1, ni)], load_sem.at[0]),
        pltpu.make_async_copy(m_in, mb, load_sem.at[1]),
        pltpu.make_async_copy(s_in, sb, load_sem.at[2]),
    ]
    for load in loads:
        load.start()

    barrier = pltpu.get_barrier_semaphore()
    pl.semaphore_signal(barrier, inc=1, device_id=peer, device_id_type=MESH)
    for there, device in beside:

        @pl.when(there)
        def _(device=device):
            pl.semaphore_signal(barrier, inc=1, device_id=device, device_id_type=MESH)

    arrivals = 1 + sum(there.astype(jnp.int32) for there, _ in beside)
    pl.semaphore_wait(barrier, arrivals)

    def rows_of(k):
        return pl.ds(k * chunk, chunk)

    def remote(src, dst, send, recv, device):
        return pltpu.make_async_remote_copy(src_ref=src, dst_ref=dst, send_sem=send, recv_sem=recv, device_id=device, device_id_type=MESH)

    def row_copy(src, t, k):
        return remote(src, rhalo.at[t, rows_of(k)], row_send.at[t, k], row_recv.at[t, k], peer)

    def boundary(t, k):
        return fb.at[lax.rem(t, 2), edge, pl.ds(1 + k * chunk, chunk)]

    def i_first(t, src=None):
        p = lax.rem(t, 2)
        src = fb.at[p, :, 1] if src is None else src
        return remote(src, fb.at[p, :, ni + 1], i_send.at[t, 0], i_recv.at[t, 1], {"cols": c - 1})

    def i_last(t, src=None):
        p = lax.rem(t, 2)
        src = fb.at[p, :, ni] if src is None else src
        return remote(src, fb.at[p, :, 0], i_send.at[t, 1], i_recv.at[t, 0], {"cols": c + 1})

    def k_first(t):
        return remote(ksend.at[t, 0], khalo.at[t, 1], k_send.at[t, 0], k_recv.at[t, 1], {"slabs": s - 1})

    def k_last(t):
        return remote(ksend.at[t, 1], khalo.at[t, 0], k_send.at[t, 1], k_recv.at[t, 0], {"slabs": s + 1})

    def first_send(k, carry):
        row_copy(f_in.at[edge, rows_of(k)], 0, k).start()
        return carry

    lax.fori_loop(0, n_chunks, first_send, 0)

    @pl.when(up)
    def _():
        i_first(0, f_in.at[:, 0]).start()

    @pl.when(down)
    def _():
        i_last(0, f_in.at[:, ni - 1]).start()

    for there, place in ((up, 0), (down, ni + 1)):

        @pl.when(jnp.logical_not(there))
        def _(place=place):
            for p in range(2):
                fb[p, :, place] = jnp.zeros((nj, nk, lanes), jnp.float32)

    for there, side in ((left, 0), (right, 1)):

        @pl.when(jnp.logical_not(there))
        def _(side=side):
            def clear(t, carry):
                khalo[t, side] = jnp.zeros((nj, ni, lanes), jnp.float32)
                return carry

            lax.fori_loop(0, STEPS, clear, 0)

    loads[0].wait()

    def first_edges(i, carry):
        for j in range(nj):
            ksend[0, 0, j, pl.ds(i, 1), :] = fb[0, j, i + 1, 0:1, :]
            ksend[0, 1, j, pl.ds(i, 1), :] = fb[0, j, i + 1, nk - 1 : nk, :]
        return carry

    lax.fori_loop(0, ni, first_edges, 0)

    def send_k(t):
        @pl.when(left)
        def _():
            k_first(t).start()

        @pl.when(right)
        def _():
            k_last(t).start()

    send_k(0)
    loads[1].wait()
    loads[2].wait()

    place = lax.broadcasted_iota(jnp.int32, (nk, lanes), 0)
    at_first, at_last = place == 0, place == nk - 1

    def step_chunk(t, k, final):
        p = lax.rem(t, 2)
        q = 1 - p
        row_copy(boundary(t, k), t, k).wait_recv()

        @pl.when(jnp.logical_and(k == 0, up))
        def _():
            i_last(t).wait_recv()

        @pl.when(jnp.logical_and(k == 0, left))
        def _():
            k_last(t).wait_recv()

        @pl.when(jnp.logical_and(k == 0, right))
        def _():
            k_first(t).wait_recv()

        @pl.when(jnp.logical_and(k == n_chunks - 1, down))
        def _():
            i_first(t).wait_recv()

        @pl.when(t >= 1)
        def _():
            row_copy(boundary(t - 1, k), t - 1, k).wait_send()

        @pl.when(jnp.logical_and(t >= 1, jnp.logical_and(k == 0, up)))
        def _():
            i_first(t - 1).wait_send()

        @pl.when(jnp.logical_and(t >= 1, jnp.logical_and(k == n_chunks - 1, down)))
        def _():
            i_last(t - 1).wait_send()

        def one_row(n, carry):
            i = k * chunk + n
            halo = rhalo[t, i]
            total = None
            for j in range(nj):
                x = fb[p, j, i + 1]
                before = fb[p, j - 1, i + 1] if j > 0 else halo * is_high
                after = fb[p, j + 1, i + 1] if j < nj - 1 else halo * is_low
                k_before = jnp.where(at_first, khalo[t, 0, j, pl.ds(i, 1), :], pltpu.roll(x, 1, 0))
                k_after = jnp.where(at_last, khalo[t, 1, j, pl.ds(i, 1), :], pltpu.roll(x, nk - 1, 0))
                spread = before + after + fb[p, j, i] + fb[p, j, i + 2] + k_before + k_after - 6.0 * x
                new = x + mb[j, i] * spread + sb[j, i]
                if final:
                    mb[j, i] = new
                    total = new if total is None else total + new
                    sb[j, i] = total * scale
                else:
                    fb[q, j, i + 1] = new
                    ksend[t + 1, 0, j, pl.ds(i, 1), :] = new[0:1]
                    ksend[t + 1, 1, j, pl.ds(i, 1), :] = new[nk - 1 : nk]
            return carry

        lax.fori_loop(0, chunk, one_row, 0)

    def step(t, carry):
        def lap(k, carry):
            step_chunk(t, k, False)
            row_copy(boundary(t + 1, k), t + 1, k).start()

            @pl.when(jnp.logical_and(k == 0, up))
            def _():
                i_first(t + 1).start()

            @pl.when(jnp.logical_and(k == n_chunks - 1, down))
            def _():
                i_last(t + 1).start()

            return carry

        lax.fori_loop(0, n_chunks, lap, 0)
        send_k(t + 1)
        return carry

    lax.fori_loop(0, STEPS - 1, step, 0)

    last = STEPS - 1

    def total_copy(k):
        return row_copy(sb.at[nj - 1, rows_of(k)], STEPS, k)

    def last_lap(k, carry):
        step_chunk(last, k, True)

        @pl.when(r == 0)
        def _():
            total_copy(k).start()

        return carry

    lax.fori_loop(0, n_chunks, last_lap, 0)

    def drain(k, carry):
        row_copy(boundary(last, k), last, k).wait_send()
        return carry

    lax.fori_loop(0, n_chunks, drain, 0)

    @pl.when(up)
    def _():
        i_first(last).wait_send()

    @pl.when(down)
    def _():
        i_last(last).wait_send()

    def drain_k(t, carry):
        @pl.when(left)
        def _():
            k_first(t).wait_send()

        @pl.when(right)
        def _():
            k_last(t).wait_send()

        return carry

    lax.fori_loop(0, STEPS, drain_k, 0)

    @pl.when(r == 0)
    def _():
        def finish(k, carry):
            total_copy(k).wait_send()
            return carry

        lax.fori_loop(0, n_chunks, finish, 0)

    @pl.when(r == 1)
    def _():
        def finish(k, carry):
            total_copy(k).wait_recv()

            def add_row(n, carry):
                i = k * chunk + n
                below = rhalo[STEPS, i]
                for j in range(nj):
                    sb[j, i] = sb[j, i] + below
                return carry

            lax.fori_loop(0, chunk, add_row, 0)
            return carry

        lax.fori_loop(0, n_chunks, finish, 0)


def flush(sums, field, sums_out, field_out, sem):
    copies = []
    for side, (src, dst) in enumerate(((sums, sums_out), (field, field_out))):
        for j in range(src.shape[0]):
            copies.append(pltpu.make_async_copy(src.at[j], dst.at[j], sem.at[side, j]))
    for copy in copies:
        copy.start()
    for copy in copies:
        copy.wait()


def fused(counts, field_values, mobility, source):
    nj, ni, nk, lanes = field_values.shape
    chunk = math.gcd(ni, 8)
    n_chunks = ni // chunk
    shape = pltpu.VMEM(field_values.shape, jnp.float32)
    dma = pltpu.SemaphoreType.DMA
    sums, field = pl.pallas_call(
        functools.partial(kernel, counts, chunk),
        out_shape=(shape, shape),
        in_specs=[pl.BlockSpec(memory_space=pl.ANY)] * 3,
        out_specs=[pl.BlockSpec(memory_space=pltpu.VMEM)] * 2,
        scratch_shapes=[
            pltpu.VMEM((2, nj, ni + 2, nk, lanes), jnp.float32),
            pltpu.VMEM((STEPS + 1, ni, nk, lanes), jnp.float32),
            pltpu.VMEM((STEPS, 2, nj, ni, lanes), jnp.float32),
            pltpu.VMEM((STEPS, 2, nj, ni, lanes), jnp.float32),
            dma((STEPS + 1, n_chunks)),
            dma((STEPS + 1, n_chunks)),
            dma((STEPS, 2)),
            dma((STEPS, 2)),
            dma((STEPS, 2)),
            dma((STEPS, 2)),
            dma((3,)),
        ],
        compiler_params=pltpu.CompilerParams(collective_id=0, has_side_effects=True, vmem_limit_bytes=32 * 1024 * 1024),
    )(field_values, mobility, source)
    result = jax.ShapeDtypeStruct(field_values.shape, jnp.float32)
    return pl.pallas_call(
        flush,
        out_shape=(result, result),
        in_specs=[pl.BlockSpec(memory_space=pltpu.VMEM)] * 2,
        out_specs=[pl.BlockSpec(memory_space=pl.ANY)] * 2,
        scratch_shapes=[dma((2, nj))],
        compiler_params=pltpu.CompilerParams(vmem_limit_bytes=18 * 1024 * 1024),
    )(sums, field)


def padded_2(array, sides, width):
    for axis, dim in sides:
        count, length = (lax.axis_size(axis), array.shape[dim])
        up = [(i, (i + 1) % count) for i in range(count - 1)]
        down = [(j, i) for i, j in up]
        last = lax.slice_in_dim(array, length - width, length, axis=dim)
        first = lax.slice_in_dim(array, 0, width, axis=dim)
        before = lax.ppermute(last, axis, up)
        after = lax.ppermute(first, axis, down)
        array = jnp.concatenate([before, array, after], axis=dim)
    return array


def prefix(array, axis, combine, identity):
    count, index = (lax.axis_size(axis), lax.axis_index(axis))
    everything = lax.all_gather(array, axis)
    start = jnp.broadcast_to(jnp.asarray(identity, array.dtype), array.shape)

    def lap(k, before):
        reached = k < index
        new = combine(before, everything[k])
        return jnp.where(reached, new, before)

    return lax.fori_loop(0, count, lap, start)


def strip_edges(values, dims):
    for dim in dims:
        values = lax.slice_in_dim(values, 1, values.shape[dim] - 1, axis=dim)
    return values


def neighbour(values, dim, start, dims):
    others = [other for other in dims if other != dim]
    values = strip_edges(values, others)
    return lax.slice_in_dim(values, start, start + values.shape[dim] - 2, axis=dim)


def one_step(padded, mobility, source):
    middle = strip_edges(padded, (0, 1, 2))
    lower = [neighbour(padded, dim, 0, (0, 1, 2)) for dim in (0, 1, 2)]
    upper = [neighbour(padded, dim, 2, (0, 1, 2)) for dim in (0, 1, 2)]
    spread = lower[0] + upper[0] + lower[1] + upper[1] + lower[2] + upper[2] - 6.0 * middle
    return middle + mobility * spread + source


def local(field_values, mobility, source):
    for step in range(STEPS):
        padded = padded_2(field_values, (("rows", 0), ("cols", 1), ("slabs", 2)), 1)
        field_values = one_step(padded, mobility, source)
    here = jnp.cumsum(field_values, axis=0)
    total = lax.slice_in_dim(here, here.shape[0] - 1, here.shape[0], axis=0)

    def add_pair(earlier_total, later_total):
        return earlier_total + later_total

    below = prefix(total, "rows", add_pair, jnp.zeros_like(total))
    column_sum = (here + below) / (field_values.shape[0] * lax.axis_size("rows"))
    return (column_sum, field_values)


def solution(mesh):
    in_specs = (
        P("rows", "cols", "slabs", None),
        P("rows", "cols", "slabs", None),
        P("rows", "cols", "slabs", None),
    )
    out_specs = (P("rows", "cols", "slabs", None), P("rows", "cols", "slabs", None))
    if mesh.shape["rows"] == 2:
        body = functools.partial(fused, tuple(mesh.shape[name] for name in ("rows", "cols", "slabs")))
    else:
        body = local
    return jax.shard_map(body, mesh=mesh, in_specs=in_specs, out_specs=out_specs, check_vma=False)
```
